32 devices in a mesh: expert: 4 (over y, x), dp: 8 (over z, core).
Axes of the slice: x: 2, y: 2, z: 4, core: 2. Of those that a mesh axis runs over, the one named last changes fastest.
Arguments:
- pool_tokens: bfloat16 [16384, 2048], P('dp', 'expert'), may hold values from -6 to 6
- pool_cotangent: bfloat16 [16384, 2048], P('dp', 'expert'), may hold values from -6 to 6
- token_ids: int32 [4, 4096], P('expert', 'dp'), may hold values from 0 to 2047, as said below
- route_weights: float32 [4, 4096], P('expert', 'dp'), may hold values from 0.1 to 1
- gate_weight: float32 [4, 2048, 512], P('expert', 'dp'), may hold values from -0.125 to 0.125
- up_weight: float32 [4, 2048, 512], P('expert', 'dp'), may hold values from -0.125 to 0.125
- down_weight: float32 [4, 512, 2048], P('expert', 'dp'), may hold values from -0.25 to 0.25
- momentum_gate: float32 [4, 2048, 512], P('expert', 'dp'), may hold values from -0.6 to 0.6
- momentum_up: float32 [4, 2048, 512], P('expert', 'dp'), may hold values from -0.6 to 0.6
- momentum_down: float32 [4, 512, 2048], P('expert', 'dp'), may hold values from -0.6 to 0.6
Outputs:
- new_gate: float32 [4, 2048, 512], P('expert', 'dp')
- new_up: float32 [4, 2048, 512], P('expert', 'dp')
- new_down: float32 [4, 512, 2048], P('expert', 'dp')
- new_momentum_gate: float32 [4, 2048, 512], P('expert', 'dp')
- new_momentum_up: float32 [4, 2048, 512], P('expert', 'dp')
- new_momentum_down: float32 [4, 512, 2048], P('expert', 'dp')
- pool_grad: float32 [16384, 2048], P('dp', 'expert')
The draws below stay inside these ranges and needn't reach their ends.
Inputs may be any that keep to these rules, and one draw needn't show every extreme that they name: `token_ids`: within one expert's 512 slots of one dp index the ids are distinct rows of that index's pool.
All inputs are finite; a program needn't handle non-finite values.
Results may differ from the reference program's by a relative error of at most 0.0066.
Values may be sent and summed in bfloat16 or wider, within the bound.
A program may use at most 128 MiB of HBM per device.

```python
import math
import jax
import jax.numpy as jnp
from jax import lax

D = 2048
H = 512
TOK_DEV = 512
POOL = 2048
EXPERTS = 4
TOKENS = 4096
POOL_ALL = 16384
N_EXPERT = 4
N_DP = 8


def draw_token_ids(key, part):
    subkeys = jax.random.split(key, N_EXPERT * N_DP)
    orders = jax.vmap(lambda single: jax.random.permutation(single, POOL)[:TOK_DEV])(subkeys)
    return orders.reshape(N_EXPERT, N_DP * TOK_DEV).astype(jnp.int32)


def draw_pool_cotangent(key, part):
    column_mean = jax.random.normal(jax.random.fold_in(key, 11), (D,), jnp.float32)
    fluctuation = jax.random.normal(jax.random.fold_in(key, 12), (N_DP * POOL, D), jnp.float32)
    values = column_mean[None, :] + 0.5 * fluctuation
    return jnp.clip(values, -6.0, 6.0).astype(jnp.bfloat16)


def block_levels(rng, extent, shards, smallest, top_value):
    def one(axis_at, shards_of):
        heights = jax.random.uniform(jax.random.fold_in(jax.random.fold_in(rng, 6), axis_at), (shards_of,), jnp.float32, smallest / len(shards), top_value / len(shards))
        return jnp.repeat(jnp.exp(heights), extent[axis_at] // shards_of).reshape((-1,) + (1,) * (len(extent) - axis_at - 1))

    gain = one(*shards[0])
    for cut in shards[1:]:
        gain = gain * one(*cut)
    return gain


def scatter_about(rng, dims, spread, reach, pieces=(), kind=jnp.bfloat16):
    factor_of = block_levels(rng, dims, pieces, -0.22, 0.18) if pieces else 1.0
    array = jax.random.normal(rng, dims, jnp.float32) * spread * factor_of
    return jnp.minimum(jnp.maximum(array, -reach), reach).astype(kind)


def setup_inputs(seed: int = 0) -> dict:
    key_list = jax.random.split(jax.random.key(seed), 11)
    return {
        "pool_tokens": scatter_about(key_list[0], (POOL_ALL, D), 1.0, 6.0, ((0, 8), (1, 4))),
        "pool_cotangent": draw_pool_cotangent(jax.random.fold_in(key_list[10], 71), 0),
        "token_ids": draw_token_ids(jax.random.fold_in(key_list[10], 71), 0),
        "route_weights": jnp.clip(jnp.exp(math.log(1.0) - 2.3025851 * jax.random.uniform(key_list[3], (EXPERTS, TOKENS), jnp.float32) ** block_levels(key_list[3], (EXPERTS, TOKENS), ((0, 4), (1, 8)), -0.2, 0.2)), 0.1, 1.0),
        "gate_weight": scatter_about(key_list[4], (EXPERTS, D, H), D ** -0.5, 0.125, ((0, 4), (1, 8)), jnp.float32),
        "up_weight": scatter_about(key_list[5], (EXPERTS, D, H), D ** -0.5, 0.125, ((0, 4), (1, 8)), jnp.float32),
        "down_weight": scatter_about(key_list[6], (EXPERTS, H, D), H ** -0.5, 0.25, ((0, 4), (1, 8)), jnp.float32),
        "momentum_gate": scatter_about(key_list[7], (EXPERTS, D, H), 0.1, 0.6, ((0, 4), (1, 8)), jnp.float32),
        "momentum_up": scatter_about(key_list[8], (EXPERTS, D, H), 0.1, 0.6, ((0, 4), (1, 8)), jnp.float32),
        "momentum_down": scatter_about(key_list[9], (EXPERTS, H, D), 0.1, 0.6, ((0, 4), (1, 8)), jnp.float32),
    }


momentum_decay = 0.9
learning_rate = 0.05
epsilon = 1e-6


def expert_terms(gate_full, up_full, down_full, pool_x, pool_c, row_ids, route):
    routed = pool_x[row_ids]
    cot_rows = pool_c[row_ids]
    gate_pre = jnp.dot(routed, gate_full, preferred_element_type=jnp.float32)
    up_pre = jnp.dot(routed, up_full, preferred_element_type=jnp.float32)
    sig = jax.nn.sigmoid(gate_pre)
    act = gate_pre * sig
    hidden = (act * up_pre).astype(jnp.bfloat16)
    scaled_cot = (route[:, None] * cot_rows.astype(jnp.float32)).astype(jnp.bfloat16)
    grad_down = lax.dot_general(hidden, scaled_cot, (((0,), (0,)), ((), ())), preferred_element_type=jnp.float32) / TOK_DEV
    hidden_grad = lax.dot_general(scaled_cot, down_full, (((1,), (1,)), ((), ())), preferred_element_type=jnp.float32)
    gate_grad = (hidden_grad * up_pre * sig * (1.0 + gate_pre * (1.0 - sig))).astype(jnp.bfloat16)
    up_grad = (hidden_grad * act).astype(jnp.bfloat16)
    grad_gate = lax.dot_general(routed, gate_grad, (((0,), (0,)), ((), ())), preferred_element_type=jnp.float32) / TOK_DEV
    grad_up = lax.dot_general(routed, up_grad, (((0,), (0,)), ((), ())), preferred_element_type=jnp.float32) / TOK_DEV
    slot_grad = lax.dot_general(gate_grad, gate_full, (((1,), (1,)), ((), ())), preferred_element_type=jnp.float32)
    slot_grad = slot_grad + lax.dot_general(up_grad, up_full, (((1,), (1,)), ((), ())), preferred_element_type=jnp.float32)
    pool_term = jax.ops.segment_sum(slot_grad, row_ids, num_segments=POOL)
    grads = jnp.stack([grad_gate.reshape(-1), grad_up.reshape(-1), grad_down.reshape(-1)])
    return grads, pool_term


def adasum_merge(left_part, right_part):
    inner = jnp.sum(left_part * right_part, axis=-1)
    norm_left = jnp.sum(left_part * left_part, axis=-1)
    norm_right = jnp.sum(right_part * right_part, axis=-1)
    coef_left = 1.0 - inner / (2.0 * (norm_left + epsilon))
    coef_right = 1.0 - inner / (2.0 * (norm_right + epsilon))
    return coef_left[..., None] * left_part + coef_right[..., None] * right_part


def reference(pool_tokens, pool_cotangent, token_ids, route_weights, gate_weight, up_weight, down_weight, momentum_gate, momentum_up, momentum_down):
    pool_x = pool_tokens.reshape(N_DP, POOL, D)
    pool_c = pool_cotangent.reshape(N_DP, POOL, D)
    tiers = N_DP.bit_length() - 1

    def per_expert(running, expert_items):
        ids_e, route_e, gate_e, up_e, down_e, mom_gate, mom_up, mom_down = expert_items
        gate_full = gate_e.astype(jnp.bfloat16)
        up_full = up_e.astype(jnp.bfloat16)
        down_full = down_e.astype(jnp.bfloat16)

        def per_device(device_items):
            return expert_terms(gate_full, up_full, down_full, device_items[0], device_items[1], device_items[2], device_items[3])

        grads, pool_terms = lax.map(per_device, (pool_x, pool_c, ids_e.reshape(N_DP, TOK_DEV), route_e.reshape(N_DP, TOK_DEV)))
        running = running + pool_terms
        merged = grads
        for tier in range(tiers):
            paired = merged.reshape(merged.shape[0] // 2, 2, 3, D * H)
            merged = adasum_merge(paired[:, 0], paired[:, 1])
        merged = merged[0]
        next_gate = momentum_decay * mom_gate + merged[0].reshape(D, H)
        next_up = momentum_decay * mom_up + merged[1].reshape(D, H)
        next_down = momentum_decay * mom_down + merged[2].reshape(H, D)
        return running, (gate_e - learning_rate * next_gate, up_e - learning_rate * next_up, down_e - learning_rate * next_down, next_gate, next_up, next_down)

    start = jnp.zeros((N_DP, POOL, D), jnp.float32)
    running, updated = lax.scan(per_expert, start, (token_ids, route_weights, gate_weight, up_weight, down_weight, momentum_gate, momentum_up, momentum_down))
    return updated[0], updated[1], updated[2], updated[3], updated[4], updated[5], running.reshape(N_DP * POOL, D)
```

```python
import jax
import jax.numpy as jnp
from jax import lax
from jax.sharding import PartitionSpec as P


momentum_decay = 0.9
learning_rate = 0.05
epsilon = 1e-06


def shift(block, axis, step):
    count = lax.axis_size(axis)
    if count & (count - 1) == 0:
        route = [(at, at ^ step) for at in range(count)]
    else:
        route = [(at, (at + step) % count) for at in range(count)]
    return lax.ppermute(block, axis, route)


def target_of(axis, step):
    count = lax.axis_size(axis)
    me = lax.axis_index(axis)
    return me ^ step if count & (count - 1) == 0 else lax.rem(me + step, count)


def source_of(axis, step):
    count = lax.axis_size(axis)
    me = lax.axis_index(axis)
    return me ^ step if count & (count - 1) == 0 else lax.rem(me - step + count, count)


def dot(left, right, dims, kind=jnp.float32):
    return lax.dot_general(
        left, right, ((dims[0], dims[1]), ((), ())), preferred_element_type=jnp.float32
    ).astype(kind)


def sums(left, right):
    cols = left.shape[-1] // 2

    def one(product):
        return [jnp.sum(product[..., :cols]), jnp.sum(product[..., cols:])]

    return one(left * right), one(left * left), one(right * right)


def coefs(inner, norm):
    return 1.0 - inner / (2.0 * (norm + epsilon))


def local(
    pool_tokens,
    pool_cotangent,
    token_ids,
    route_weights,
    gate_weight,
    up_weight,
    down_weight,
    momentum_gate,
    momentum_up,
    momentum_down,
):
    bf16, f32 = jnp.bfloat16, jnp.float32
    n_e = lax.axis_size("expert")
    n_dp = lax.axis_size("dp")
    pool_rows, width = pool_tokens.shape
    slots = token_ids.shape[1]
    hid = gate_weight.shape[2]
    all_ids = lax.all_gather(token_ids[0], "expert", axis=0)
    shard_gu = jnp.concatenate([gate_weight[0], up_weight[0]], axis=1).astype(bf16)
    gu_full = lax.all_gather(shard_gu, "dp", axis=0, tiled=True)
    down_full = lax.all_gather(down_weight[0].astype(bf16), "dp", axis=0, tiled=True)

    pool = jnp.concatenate([pool_tokens, pool_cotangent], axis=1)
    rows = lax.iota(jnp.int32, pool_rows)

    def picked(owner):
        ids = lax.dynamic_index_in_dim(all_ids, owner, 0, keepdims=False)
        return dot((ids[:, None] == rows[None, :]).astype(bf16), pool, ((1,), (0,)), bf16)

    me_e = lax.axis_index("expert")
    arrived = []
    for step in range(1, n_e):
        arrived.append((source_of("expert", step), shift(picked(target_of("expert", step)), "expert", step)))
    arrived.append((me_e, picked(me_e)))
    routed = jnp.zeros((slots, n_e * width), bf16)
    cot_rows = jnp.zeros((slots, n_e * width), bf16)
    for owner, block in arrived:
        routed = lax.dynamic_update_slice(routed, block[:, :width], (0, owner * width))
        cot_rows = lax.dynamic_update_slice(cot_rows, block[:, width:], (0, owner * width))

    route = route_weights[0]
    scaled_cot = (route[:, None] * cot_rows.astype(f32)).astype(bf16)
    pre = dot(routed, gu_full, ((1,), (0,)))
    gate_pre, up_pre = pre[:, :hid], pre[:, hid:]
    sig = jax.nn.sigmoid(gate_pre)
    act = gate_pre * sig
    hidden = (act * up_pre).astype(bf16)
    hidden_grad = dot(scaled_cot, down_full, ((1,), (1,)))
    gate_grad = (hidden_grad * up_pre * sig * (1.0 + gate_pre * (1.0 - sig))).astype(bf16)
    up_grad = (hidden_grad * act).astype(bf16)
    both_grad = jnp.concatenate([gate_grad, up_grad], axis=1)

    me = lax.axis_index("dp")
    tiers = n_dp.bit_length() - 1
    own_bit = me & 1
    rows_gu = gate_weight.shape[1]
    rows_d = down_weight.shape[1]
    routed_v = routed.reshape(slots, n_dp // 2, 2, rows_gu)
    hidden_v = hidden.reshape(slots, n_dp // 2, 2, rows_d)

    def half(bit, kind):
        left = lax.dynamic_index_in_dim(routed_v, bit, 2, keepdims=False).reshape(slots, -1)
        left_d = lax.dynamic_index_in_dim(hidden_v, bit, 2, keepdims=False).reshape(slots, -1)
        gu = (dot(left, both_grad, ((0,), (0,))) / slots).astype(kind)
        dn = (dot(left_d, scaled_cot, ((0,), (0,))) / slots).astype(kind)
        return gu.reshape(n_dp // 2, rows_gu, -1), dn.reshape(n_dp // 2, rows_d, -1)

    sent = half(1 - own_bit, bf16)
    got = [shift(part, "dp", 1) for part in sent]

    returned = [None] * n_e
    for step in range(1, n_e):
        rows_w = lax.dynamic_slice_in_dim(gu_full, target_of("expert", step) * width, width, 0)
        part = dot(both_grad, rows_w, ((1,), (1,)), bf16)
        returned[step] = shift(part, "expert", step)
    rows_w = lax.dynamic_slice_in_dim(gu_full, me_e * width, width, 0)
    returned[0] = dot(both_grad, rows_w, ((1,), (1,)), bf16)

    kept = half(own_bit, f32)
    for tier in range(tiers):
        bit = me >> tier & 1
        if tier:
            views = [part.reshape(part.shape[0] // 2, 2, *part.shape[1:]) for part in kept]
            got = [
                shift(lax.dynamic_index_in_dim(v, 1 - bit, 1, keepdims=False).astype(bf16), "dp", 1 << tier)
                for v in views
            ]
            kept = [lax.dynamic_index_in_dim(v, bit, 1, keepdims=False) for v in views]
        got = [part.astype(f32) for part in got]
        inner, mine, other = sums(kept[0], got[0])
        flat = jnp.stack(
            [*inner, jnp.sum(kept[1] * got[1]), *mine, jnp.sum(kept[1] * kept[1]), *other, jnp.sum(got[1] * got[1])]
        ).reshape(3, 3)
        left_first = jnp.where(bit == 0, flat, jnp.stack([flat[0], flat[2], flat[1]]))
        total = left_first
        for level in range(tier + 1):
            total = total + shift(total, "dp", 1 << level)
        c_left, c_right = coefs(total[0], total[1]), coefs(total[0], total[2])
        c_mine = jnp.where(bit == 0, c_left, c_right)
        c_other = jnp.where(bit == 0, c_right, c_left)
        col_mine = jnp.concatenate([jnp.broadcast_to(c_mine[0], (hid,)), jnp.broadcast_to(c_mine[1], (hid,))])
        col_other = jnp.concatenate([jnp.broadcast_to(c_other[0], (hid,)), jnp.broadcast_to(c_other[1], (hid,))])
        kept = [
            kept[0] * col_mine + got[0] * col_other,
            kept[1] * c_mine[2] + got[1] * c_other[2],
        ]

    owners = jnp.stack([source_of("expert", step) if step else me_e for step in range(n_e)])
    ids_back = all_ids[owners].reshape(-1)
    pool_grad = dot(
        (rows[:, None] == ids_back[None, :]).astype(bf16), jnp.concatenate(returned, axis=0), ((1,), (0,))
    )

    next_gate = momentum_decay * momentum_gate[0] + kept[0][0, :, :hid]
    next_up = momentum_decay * momentum_up[0] + kept[0][0, :, hid:]
    next_down = momentum_decay * momentum_down[0] + kept[1][0]
    new_gate = gate_weight[0] - learning_rate * next_gate
    new_up = up_weight[0] - learning_rate * next_up
    new_down = down_weight[0] - learning_rate * next_down
    return (
        new_gate[None],
        new_up[None],
        new_down[None],
        next_gate[None],
        next_up[None],
        next_down[None],
        pool_grad,
    )


def solution(mesh):
    in_specs = (
        P("dp", "expert"),
        P("dp", "expert"),
        P("expert", "dp"),
        P("expert", "dp"),
        P("expert", "dp", None),
        P("expert", "dp", None),
        P("expert", "dp", None),
        P("expert", "dp", None),
        P("expert", "dp", None),
        P("expert", "dp", None),
    )
    out_specs = (
        P("expert", "dp", None),
        P("expert", "dp", None),
        P("expert", "dp", None),
        P("expert", "dp", None),
        P("expert", "dp", None),
        P("expert", "dp", None),
        P("dp", "expert"),
    )
    return jax.shard_map(local, mesh=mesh, in_specs=in_specs, out_specs=out_specs, check_vma=False)
```

```python
import functools

import jax
import jax.numpy as jnp
from jax import lax
from jax.experimental import pallas as pl
from jax.experimental.pallas import tpu as pltpu
from jax.sharding import PartitionSpec as P


momentum_decay = 0.9
learning_rate = 0.05
epsilon = 1e-06


def shift(block, axis, step):
    count = lax.axis_size(axis)
    if count & (count - 1) == 0:
        route = [(at, at ^ step) for at in range(count)]
    else:
        route = [(at, (at + step) % count) for at in range(count)]
    return lax.ppermute(block, axis, route)


def target_of(axis, step):
    count = lax.axis_size(axis)
    me = lax.axis_index(axis)
    return me ^ step if count & (count - 1) == 0 else lax.rem(me + step, count)


def source_of(axis, step):
    count = lax.axis_size(axis)
    me = lax.axis_index(axis)
    return me ^ step if count & (count - 1) == 0 else lax.rem(me - step + count, count)


def dot(left, right, dims, kind=jnp.float32):
    return lax.dot_general(
        left, right, ((dims[0], dims[1]), ((), ())), preferred_element_type=jnp.float32
    ).astype(kind)


def coefs(inner, norm):
    return 1.0 - inner / (2.0 * (norm + epsilon))


def merge_kernel(
    n_e, n_dp, hid,
    sent_gu, sent_dn, kept_gu, kept_dn, slot_grad, ids,
    pool_out, gu_out, dn_out,
    returned, stats, stats_in, own_gu, own_dn, out_gu, out_dn, in_gu, in_dn,
    ret_send, ret_recv, blk_send, blk_recv, st_send, st_recv,
):
    f32, bf16 = jnp.float32, jnp.bfloat16
    MESH = pl.DeviceIdType.MESH
    me, me_e = lax.axis_index("dp"), lax.axis_index("expert")
    tiers = n_dp.bit_length() - 1
    slots = slot_grad.shape[0]
    width = slot_grad.shape[1] // n_e
    rows_gu, rows_dn = kept_gu.shape[1], kept_dn.shape[1]
    step_rows = 16

    barrier = pltpu.get_barrier_semaphore()
    for d in range(1, n_dp):
        pl.semaphore_signal(barrier, inc=1, device_id={"dp": me ^ d}, device_id_type=MESH)
    for d in range(1, n_e):
        pl.semaphore_signal(barrier, inc=1, device_id={"expert": me_e ^ d}, device_id_type=MESH)
    pl.semaphore_wait(barrier, n_dp + n_e - 2)

    pending = []

    def send(src, dst, ssem, rsem, device):
        copy = pltpu.make_async_remote_copy(
            src_ref=src, dst_ref=dst, send_sem=ssem, recv_sem=rsem, device_id=device, device_id_type=MESH
        )
        copy.start()
        pending.append(copy)
        return copy

    offset, start = [], 0
    for tier in range(tiers):
        offset.append(start)
        start += 2 * (n_dp >> (tier + 1))

    def send_block(tier, j):
        peer = {"dp": me ^ (1 << tier)}
        src_gu, src_dn = (sent_gu, sent_dn) if tier == 0 else (out_gu[tier - 1], out_dn[tier - 1])
        at = offset[tier] + 2 * j
        return (
            send(src_gu.at[j], in_gu[tier].at[j], blk_send.at[at], blk_recv.at[at], peer),
            send(src_dn.at[j], in_dn[tier].at[j], blk_send.at[at + 1], blk_recv.at[at + 1], peer),
        )

    flying = [send_block(0, j) for j in range(n_dp // 2)]
    back = [None]
    for d in range(1, n_e):
        col = pl.multiple_of((me_e ^ d) * width, width)
        back.append(
            send(
                slot_grad.at[:, pl.ds(col, width)],
                returned.at[pl.ds(d * slots, slots)],
                ret_send.at[d], ret_recv.at[d], {"expert": me_e ^ d},
            )
        )
    returned[pl.ds(0, slots), :] = slot_grad[:, pl.ds(pl.multiple_of(me_e * width, width), width)]

    def pool_sum():
        for copy in back[1:]:
            copy.wait_recv()
        tile = 256

        @pl.loop(0, pool_out.shape[0] // tile)
        def _(t):
            at = pl.multiple_of(t * tile, tile)
            row = lax.broadcasted_iota(jnp.int32, (tile, n_e * slots), 0) + at
            pick = jnp.where(row == ids[...], 1.0, 0.0).astype(bf16)
            pool_out[pl.ds(at, tile), :] = jnp.dot(pick, returned[...], preferred_element_type=f32)

    def accumulate(mine, other, rows, j, acc):
        def body(t, acc):
            at = pl.ds(pl.multiple_of(t * step_rows, step_rows), step_rows)
            a = mine[j, at, :]
            b = other[j, at, :].astype(f32)

            def fold(x):
                return x[:8] + x[8:]

            return acc[0] + fold(a * b), acc[1] + fold(a * a), acc[2] + fold(b * b)

        return lax.fori_loop(0, rows // step_rows, body, acc)

    def lanes(x):
        total = x[:, :128]
        for c in range(1, x.shape[1] // 128):
            total = total + x[:, c * 128 : (c + 1) * 128]
        return jnp.sum(total, axis=0, keepdims=True)

    mine_gu, mine_dn = kept_gu, kept_dn
    for tier in range(tiers):
        blocks = n_dp >> (tier + 1)
        bit = (me >> tier) & 1
        if tier == tiers - 1:
            pool_sum()
        acc_gu = tuple(jnp.zeros((8, 2 * hid), f32) for _ in range(3))
        acc_dn = tuple(jnp.zeros((8, kept_dn.shape[2]), f32) for _ in range(3))
        for j in range(blocks):
            flying[j][0].wait_recv()
            acc_gu = accumulate(mine_gu, in_gu[tier], rows_gu, j, acc_gu)
        for j in range(blocks):
            flying[j][1].wait_recv()
            acc_dn = accumulate(mine_dn, in_dn[tier], rows_dn, j, acc_dn)
        parts = [[lanes(acc_gu[i][:, :hid]), lanes(acc_gu[i][:, hid:]), lanes(acc_dn[i])] for i in range(3)]
        left = [jnp.where(bit == 0, m, o) for m, o in zip(parts[1], parts[2])]
        right = [jnp.where(bit == 0, o, m) for m, o in zip(parts[1], parts[2])]
        local_stats = jnp.concatenate(
            [*parts[0], *left, *right, jnp.zeros((7, 128), f32)], axis=0
        )
        stats[tier] = local_stats
        group = 2 << tier
        first = group - 2 - tier
        news = [
            send(
                stats.at[tier], stats_in.at[first + d - 1],
                st_send.at[first + d - 1], st_recv.at[first + d - 1], {"dp": me ^ d},
            )
            for d in range(1, group)
        ]
        total = local_stats
        for d in range(1, group):
            news[d - 1].wait_recv()
            total = total + stats_in[first + d - 1]
        whole = jnp.sum(total, axis=1, keepdims=True)
        inner = whole[0:3]
        c_left, c_right = coefs(inner, whole[3:6]), coefs(inner, whole[6:9])
        c_mine = jnp.where(bit == 0, c_left, c_right)
        c_other = jnp.where(bit == 0, c_right, c_left)

        def spread(c):
            return jnp.concatenate(
                [jnp.broadcast_to(c[0:1], (1, hid)), jnp.broadcast_to(c[1:2], (1, hid))], axis=1
            ), c[2:3]

        (gu_m, dn_m), (gu_o, dn_o) = spread(c_mine), spread(c_other)

        def combine(mine, other, rows, j, c_m, c_o, store):
            def body(t, carry):
                at = pl.ds(pl.multiple_of(t * step_rows, step_rows), step_rows)
                store(at, mine[j, at, :] * c_m + other[j, at, :].astype(f32) * c_o)
                return carry

            lax.fori_loop(0, rows // step_rows, body, 0)

        def storer(ref, j):
            def store(at, value):
                ref[j, at, :] = value.astype(ref.dtype)

            return store

        def store_gu(at, value):
            gu_out[at, :] = value

        def store_dn(at, value):
            dn_out[at, :] = value

        if tier == tiers - 1:
            combine(mine_gu, in_gu[tier], rows_gu, 0, gu_m, gu_o, store_gu)
            combine(mine_dn, in_dn[tier], rows_dn, 0, dn_m, dn_o, store_dn)
        else:
            up = (me >> (tier + 1)) & 1
            flying = []
            for j in range(blocks // 2):
                combine(mine_gu, in_gu[tier], rows_gu, 2 * j + 1 - up, gu_m, gu_o, storer(out_gu[tier], j))
                combine(mine_dn, in_dn[tier], rows_dn, 2 * j + 1 - up, dn_m, dn_o, storer(out_dn[tier], j))
                flying.append(send_block(tier + 1, j))
            for j in range(blocks // 2):
                combine(mine_gu, in_gu[tier], rows_gu, 2 * j + up, gu_m, gu_o, storer(own_gu[tier], j))
                combine(mine_dn, in_dn[tier], rows_dn, 2 * j + up, dn_m, dn_o, storer(own_dn[tier], j))
            mine_gu, mine_dn = own_gu[tier], own_dn[tier]
    for copy in pending:
        copy.wait_send()


def merged(sent, kept, slot_grad, ids_back, pool_rows, n_e, n_dp, hid):
    f32, bf16 = jnp.float32, jnp.bfloat16
    gu, dn = kept[0].shape[1:], kept[1].shape[1:]
    slots, full = slot_grad.shape
    tiers = n_dp.bit_length() - 1
    n_blocks = sum(2 * (n_dp >> (t + 1)) for t in range(tiers))
    n_stats = sum((2 << t) - 1 for t in range(tiers))
    vmem = pl.BlockSpec(memory_space=pltpu.VMEM)

    def per_tier(shape, kind, first):
        return [pltpu.VMEM((n_dp >> (t + 1), *shape), kind) for t in range(first, tiers)]

    return pl.pallas_call(
        functools.partial(merge_kernel, n_e, n_dp, hid),
        out_shape=(
            jax.ShapeDtypeStruct((pool_rows, full // n_e), f32),
            jax.ShapeDtypeStruct(gu, f32),
            jax.ShapeDtypeStruct(dn, f32),
        ),
        in_specs=[vmem] * 6,
        out_specs=(vmem,) * 3,
        scratch_shapes=[
            pltpu.VMEM((n_e * slots, full // n_e), bf16),
            pltpu.VMEM((tiers, 16, 128), f32),
            pltpu.VMEM((n_stats, 16, 128), f32),
            per_tier(gu, f32, 1),
            per_tier(dn, f32, 1),
            per_tier(gu, bf16, 1),
            per_tier(dn, bf16, 1),
            per_tier(gu, bf16, 0),
            per_tier(dn, bf16, 0),
            pltpu.SemaphoreType.DMA((n_e,)),
            pltpu.SemaphoreType.DMA((n_e,)),
            pltpu.SemaphoreType.DMA((n_blocks,)),
            pltpu.SemaphoreType.DMA((n_blocks,)),
            pltpu.SemaphoreType.DMA((n_stats,)),
            pltpu.SemaphoreType.DMA((n_stats,)),
        ],
        compiler_params=pltpu.CompilerParams(
            collective_id=1, has_side_effects=True, vmem_limit_bytes=60 * 1024 * 1024
        ),
    )(sent[0], sent[1], kept[0], kept[1], slot_grad, ids_back)


def local(
    pool_tokens,
    pool_cotangent,
    token_ids,
    route_weights,
    gate_weight,
    up_weight,
    down_weight,
    momentum_gate,
    momentum_up,
    momentum_down,
):
    bf16, f32 = jnp.bfloat16, jnp.float32
    n_e = lax.axis_size("expert")
    n_dp = lax.axis_size("dp")
    pool_rows, width = pool_tokens.shape
    slots = token_ids.shape[1]
    hid = gate_weight.shape[2]
    all_ids = lax.all_gather(token_ids[0], "expert", axis=0)
    shard_gu = jnp.concatenate([gate_weight[0], up_weight[0]], axis=1).astype(bf16)
    gu_full = lax.all_gather(shard_gu, "dp", axis=0, tiled=True)
    down_full = lax.all_gather(down_weight[0].astype(bf16), "dp", axis=0, tiled=True)

    pool = jnp.concatenate([pool_tokens, pool_cotangent], axis=1)
    rows = lax.iota(jnp.int32, pool_rows)

    def picked(owner):
        ids = lax.dynamic_index_in_dim(all_ids, owner, 0, keepdims=False)
        return dot((ids[:, None] == rows[None, :]).astype(bf16), pool, ((1,), (0,)), bf16)

    me_e = lax.axis_index("expert")
    arrived = []
    for step in range(1, n_e):
        arrived.append((source_of("expert", step), shift(picked(target_of("expert", step)), "expert", step)))
    arrived.append((me_e, picked(me_e)))
    routed = jnp.zeros((slots, n_e * width), bf16)
    cot_rows = jnp.zeros((slots, n_e * width), bf16)
    for owner, block in arrived:
        routed = lax.dynamic_update_slice(routed, block[:, :width], (0, owner * width))
        cot_rows = lax.dynamic_update_slice(cot_rows, block[:, width:], (0, owner * width))

    route = route_weights[0]
    scaled_cot = (route[:, None] * cot_rows.astype(f32)).astype(bf16)
    pre = dot(routed, gu_full, ((1,), (0,)))
    gate_pre, up_pre = pre[:, :hid], pre[:, hid:]
    sig = jax.nn.sigmoid(gate_pre)
    act = gate_pre * sig
    hidden = (act * up_pre).astype(bf16)
    hidden_grad = dot(scaled_cot, down_full, ((1,), (1,)))
    gate_grad = (hidden_grad * up_pre * sig * (1.0 + gate_pre * (1.0 - sig))).astype(bf16)
    up_grad = (hidden_grad * act).astype(bf16)
    both_grad = jnp.concatenate([gate_grad, up_grad], axis=1)

    me = lax.axis_index("dp")
    own_bit = me & 1
    rows_gu = gate_weight.shape[1]
    rows_d = down_weight.shape[1]
    routed_v = routed.reshape(slots, n_dp // 2, 2, rows_gu)
    hidden_v = hidden.reshape(slots, n_dp // 2, 2, rows_d)

    def half(bit, kind):
        left = lax.dynamic_index_in_dim(routed_v, bit, 2, keepdims=False).reshape(slots, -1)
        left_d = lax.dynamic_index_in_dim(hidden_v, bit, 2, keepdims=False).reshape(slots, -1)
        gu = (dot(left, both_grad, ((0,), (0,))) / slots).astype(kind)
        dn = (dot(left_d, scaled_cot, ((0,), (0,))) / slots).astype(kind)
        return gu.reshape(n_dp // 2, rows_gu, -1), dn.reshape(n_dp // 2, rows_d, -1)

    sent = half(1 - own_bit, bf16)
    kept = half(own_bit, f32)
    slot_grad = dot(both_grad, gu_full, ((1,), (1,)), bf16)
    owners = jnp.stack([me_e ^ step for step in range(n_e)])
    ids_back = all_ids[owners].reshape(1, -1)
    pool_grad, fin_gu, fin_dn = merged(sent, kept, slot_grad, ids_back, pool_rows, n_e, n_dp, hid)

    next_gate = momentum_decay * momentum_gate[0] + fin_gu[:, :hid]
    next_up = momentum_decay * momentum_up[0] + fin_gu[:, hid:]
    next_down = momentum_decay * momentum_down[0] + fin_dn
    new_gate = gate_weight[0] - learning_rate * next_gate
    new_up = up_weight[0] - learning_rate * next_up
    new_down = down_weight[0] - learning_rate * next_down
    return (
        new_gate[None],
        new_up[None],
        new_down[None],
        next_gate[None],
        next_up[None],
        next_down[None],
        pool_grad,
    )


def solution(mesh):
    in_specs = (
        P("dp", "expert"),
        P("dp", "expert"),
        P("expert", "dp"),
        P("expert", "dp"),
        P("expert", "dp", None),
        P("expert", "dp", None),
        P("expert", "dp", None),
        P("expert", "dp", None),
        P("expert", "dp", None),
        P("expert", "dp", None),
    )
    out_specs = (
        P("expert", "dp", None),
        P("expert", "dp", None),
        P("expert", "dp", None),
        P("expert", "dp", None),
        P("expert", "dp", None),
        P("expert", "dp", None),
        P("dp", "expert"),
    )
    return jax.shard_map(local, mesh=mesh, in_specs=in_specs, out_specs=out_specs, check_vma=False)
```

```python
import functools

import jax
import jax.numpy as jnp
from jax import lax
from jax.experimental import pallas as pl
from jax.experimental.pallas import tpu as pltpu
from jax.sharding import PartitionSpec as P


momentum_decay = 0.9
learning_rate = 0.05
epsilon = 1e-06

def dot(left, right, dims, kind=jnp.float32):
    return lax.dot_general(
        left, right, ((dims[0], dims[1]), ((), ())), preferred_element_type=jnp.float32
    ).astype(kind)


def coefs(inner, norm):
    return 1.0 - inner / (2.0 * (norm + epsilon))


def merge_kernel(
    n_e, n_dp, hid,
    sent_gu, sent_dn, kept_gu, kept_dn, slot_grad, ids,
    pool_out, gu_out, dn_out,
    returned, stats, stats_in, own_gu, own_dn, out_gu, out_dn, in_gu, in_dn,
    ret_send, ret_recv, blk_send, blk_recv, st_send, st_recv,
):
    f32, bf16 = jnp.float32, jnp.bfloat16
    MESH = pl.DeviceIdType.MESH
    me, me_e = lax.axis_index("dp"), lax.axis_index("expert")
    tiers = n_dp.bit_length() - 1
    slots = slot_grad.shape[0]
    width = slot_grad.shape[1] // n_e
    rows_gu, rows_dn = kept_gu.shape[1], kept_dn.shape[1]
    step_rows = 16

    barrier = pltpu.get_barrier_semaphore()
    for d in range(1, n_dp):
        pl.semaphore_signal(barrier, inc=1, device_id={"dp": me ^ d}, device_id_type=MESH)
    for d in range(1, n_e):
        pl.semaphore_signal(barrier, inc=1, device_id={"expert": me_e ^ d}, device_id_type=MESH)
    pl.semaphore_wait(barrier, n_dp + n_e - 2)

    pending = []

    def send(src, dst, ssem, rsem, device):
        copy = pltpu.make_async_remote_copy(
            src_ref=src, dst_ref=dst, send_sem=ssem, recv_sem=rsem, device_id=device, device_id_type=MESH
        )
        copy.start()
        pending.append(copy)
        return copy

    offset, start = [], 0
    for tier in range(tiers):
        offset.append(start)
        start += 2 * (n_dp >> (tier + 1))

    def send_block(tier, j):
        peer = {"dp": me ^ (1 << tier)}
        src_gu, src_dn = (sent_gu, sent_dn) if tier == 0 else (out_gu[tier - 1], out_dn[tier - 1])
        at = offset[tier] + 2 * j
        return (
            send(src_gu.at[j], in_gu[tier].at[j], blk_send.at[at], blk_recv.at[at], peer),
            send(src_dn.at[j], in_dn[tier].at[j], blk_send.at[at + 1], blk_recv.at[at + 1], peer),
        )

    flying = [send_block(0, j) for j in range(n_dp // 2)]
    back = [None]
    for d in range(1, n_e):
        col = pl.multiple_of((me_e ^ d) * width, width)
        back.append(
            send(
                slot_grad.at[:, pl.ds(col, width)],
                returned.at[pl.ds(d * slots, slots)],
                ret_send.at[d], ret_recv.at[d], {"expert": me_e ^ d},
            )
        )
    returned[pl.ds(0, slots), :] = slot_grad[:, pl.ds(pl.multiple_of(me_e * width, width), width)]

    def pool_sum():
        for copy in back[1:]:
            copy.wait_recv()
        tile = 256

        @pl.loop(0, pool_out.shape[0] // tile)
        def _(t):
            at = pl.multiple_of(t * tile, tile)
            row = lax.broadcasted_iota(jnp.int32, (tile, n_e * slots), 0) + at
            pick = jnp.where(row == ids[...], 1.0, 0.0).astype(bf16)
            pool_out[pl.ds(at, tile), :] = jnp.dot(pick, returned[...], preferred_element_type=f32)

    def accumulate(mine, other, rows, j, acc):
        def body(t, acc):
            at = pl.ds(pl.multiple_of(t * step_rows, step_rows), step_rows)
            a = mine[j, at, :]
            b = other[j, at, :].astype(f32)

            def fold(x):
                return x[:8] + x[8:]

            return acc[0] + fold(a * b), acc[1] + fold(a * a), acc[2] + fold(b * b)

        return lax.fori_loop(0, rows // step_rows, body, acc)

    def lanes(x):
        total = x[:, :128]
        for c in range(1, x.shape[1] // 128):
            total = total + x[:, c * 128 : (c + 1) * 128]
        return jnp.sum(total, axis=0, keepdims=True)

    mine_gu, mine_dn = kept_gu, kept_dn
    for tier in range(tiers):
        blocks = n_dp >> (tier + 1)
        bit = (me >> tier) & 1
        if tier == tiers - 1:
            pool_sum()
        acc_gu = tuple(jnp.zeros((8, 2 * hid), f32) for _ in range(3))
        acc_dn = tuple(jnp.zeros((8, kept_dn.shape[2]), f32) for _ in range(3))
        for j in range(blocks):
            flying[j][0].wait_recv()
            acc_gu = accumulate(mine_gu, in_gu[tier], rows_gu, j, acc_gu)
        for j in range(blocks):
            flying[j][1].wait_recv()
            acc_dn = accumulate(mine_dn, in_dn[tier], rows_dn, j, acc_dn)
        parts = [[lanes(acc_gu[i][:, :hid]), lanes(acc_gu[i][:, hid:]), lanes(acc_dn[i])] for i in range(3)]
        left = [jnp.where(bit == 0, m, o) for m, o in zip(parts[1], parts[2])]
        right = [jnp.where(bit == 0, o, m) for m, o in zip(parts[1], parts[2])]
        local_stats = jnp.concatenate(
            [*parts[0], *left, *right, jnp.zeros((7, 128), f32)], axis=0
        )
        stats[tier] = local_stats
        group = 2 << tier
        first = group - 2 - tier
        news = [
            send(
                stats.at[tier], stats_in.at[first + d - 1],
                st_send.at[first + d - 1], st_recv.at[first + d - 1], {"dp": me ^ d},
            )
            for d in range(1, group)
        ]
        total = local_stats
        for d in range(1, group):
            news[d - 1].wait_recv()
            total = total + stats_in[first + d - 1]
        whole = jnp.sum(total, axis=1, keepdims=True)
        inner = whole[0:3]
        c_left, c_right = coefs(inner, whole[3:6]), coefs(inner, whole[6:9])
        c_mine = jnp.where(bit == 0, c_left, c_right)
        c_other = jnp.where(bit == 0, c_right, c_left)

        def spread(c):
            return jnp.concatenate(
                [jnp.broadcast_to(c[0:1], (1, hid)), jnp.broadcast_to(c[1:2], (1, hid))], axis=1
            ), c[2:3]

        (gu_m, dn_m), (gu_o, dn_o) = spread(c_mine), spread(c_other)

        def combine(mine, other, rows, j, c_m, c_o, store):
            def body(t, carry):
                at = pl.ds(pl.multiple_of(t * step_rows, step_rows), step_rows)
                store(at, mine[j, at, :] * c_m + other[j, at, :].astype(f32) * c_o)
                return carry

            lax.fori_loop(0, rows // step_rows, body, 0)

        def storer(ref, j):
            def store(at, value):
                ref[j, at, :] = value.astype(ref.dtype)

            return store

        def store_gu(at, value):
            gu_out[at, :] = value

        def store_dn(at, value):
            dn_out[at, :] = value

        if tier == tiers - 1:
            combine(mine_gu, in_gu[tier], rows_gu, 0, gu_m, gu_o, store_gu)
            combine(mine_dn, in_dn[tier], rows_dn, 0, dn_m, dn_o, store_dn)
        else:
            up = (me >> (tier + 1)) & 1
            flying = []
            for j in range(blocks // 2):
                combine(mine_gu, in_gu[tier], rows_gu, 2 * j + 1 - up, gu_m, gu_o, storer(out_gu[tier], j))
                combine(mine_dn, in_dn[tier], rows_dn, 2 * j + 1 - up, dn_m, dn_o, storer(out_dn[tier], j))
                flying.append(send_block(tier + 1, j))
            for j in range(blocks // 2):
                combine(mine_gu, in_gu[tier], rows_gu, 2 * j + up, gu_m, gu_o, storer(own_gu[tier], j))
                combine(mine_dn, in_dn[tier], rows_dn, 2 * j + up, dn_m, dn_o, storer(own_dn[tier], j))
            mine_gu, mine_dn = own_gu[tier], own_dn[tier]
    for copy in pending:
        copy.wait_send()


def merged(sent, kept, slot_grad, ids_back, pool_rows, n_e, n_dp, hid):
    f32, bf16 = jnp.float32, jnp.bfloat16
    gu, dn = kept[0].shape[1:], kept[1].shape[1:]
    slots, full = slot_grad.shape
    tiers = n_dp.bit_length() - 1
    n_blocks = sum(2 * (n_dp >> (t + 1)) for t in range(tiers))
    n_stats = sum((2 << t) - 1 for t in range(tiers))
    vmem = pl.BlockSpec(memory_space=pltpu.VMEM)

    def per_tier(shape, kind, first):
        return [pltpu.VMEM((n_dp >> (t + 1), *shape), kind) for t in range(first, tiers)]

    return pl.pallas_call(
        functools.partial(merge_kernel, n_e, n_dp, hid),
        out_shape=(
            jax.ShapeDtypeStruct((pool_rows, full // n_e), f32),
            jax.ShapeDtypeStruct(gu, f32),
            jax.ShapeDtypeStruct(dn, f32),
        ),
        in_specs=[vmem] * 6,
        out_specs=(vmem,) * 3,
        scratch_shapes=[
            pltpu.VMEM((n_e * slots, full // n_e), bf16),
            pltpu.VMEM((tiers, 16, 128), f32),
            pltpu.VMEM((n_stats, 16, 128), f32),
            per_tier(gu, f32, 1),
            per_tier(dn, f32, 1),
            per_tier(gu, bf16, 1),
            per_tier(dn, bf16, 1),
            per_tier(gu, bf16, 0),
            per_tier(dn, bf16, 0),
            pltpu.SemaphoreType.DMA((n_e,)),
            pltpu.SemaphoreType.DMA((n_e,)),
            pltpu.SemaphoreType.DMA((n_blocks,)),
            pltpu.SemaphoreType.DMA((n_blocks,)),
            pltpu.SemaphoreType.DMA((n_stats,)),
            pltpu.SemaphoreType.DMA((n_stats,)),
        ],
        compiler_params=pltpu.CompilerParams(
            collective_id=1, has_side_effects=True, vmem_limit_bytes=60 * 1024 * 1024
        ),
    )(sent[0], sent[1], kept[0], kept[1], slot_grad, ids_back)


def gather_kernel(
    n_e, n_dp,
    ids, tokens, cot, shard_gu, shard_dn,
    routed, cot_rows, gu_full, dn_full, all_ids,
    stage_x, stage_c,
    id_send, id_recv, tok_send, tok_recv, line_send, line_recv, pair_send, pair_recv,
):
    f32, bf16 = jnp.float32, jnp.bfloat16
    MESH = pl.DeviceIdType.MESH
    me, me_e = lax.axis_index("dp"), lax.axis_index("expert")
    chips = n_dp // 2
    chip, core = me // 2, me % 2
    slots = ids.shape[1]
    pool_rows, width = tokens.shape

    barrier = pltpu.get_barrier_semaphore()
    for d in range(1, n_e):
        pl.semaphore_signal(barrier, inc=1, device_id={"expert": me_e ^ d}, device_id_type=MESH)
    pl.semaphore_signal(barrier, inc=1, device_id={"dp": me ^ 1}, device_id_type=MESH)
    for way in (-1, 1):
        pl.semaphore_signal(
            barrier, inc=1, device_id={"dp": lax.rem(me + 2 * way + n_dp, n_dp)}, device_id_type=MESH
        )
    pl.semaphore_wait(barrier, n_e + 2)

    def remote(src, dst, ssem, rsem, device):
        return pltpu.make_async_remote_copy(
            src_ref=src, dst_ref=dst, send_sem=ssem, recv_sem=rsem, device_id=device, device_id_type=MESH
        )

    pending = []
    id_copies = [None]
    for d in range(1, n_e):
        copy = remote(ids, all_ids.at[d], id_send.at[d], id_recv.at[d], {"expert": me_e ^ d})
        copy.start()
        id_copies.append(copy)
        pending.append(copy)
    all_ids[0] = ids[...]

    fulls = (gu_full, dn_full)
    shards = (shard_gu, shard_dn)

    def along(way, hop, part):
        side = 0 if way > 0 else 1
        origin = me - 2 * way * hop
        src = shards[part] if hop == 0 else fulls[part].at[origin]
        return remote(
            src, fulls[part].at[origin],
            line_send.at[side, hop, part], line_recv.at[side, hop, part], {"dp": me + 2 * way},
        )

    def arriving(way, hop, part):
        side = 0 if way > 0 else 1
        origin = me - 2 * way * (hop + 1)
        return remote(
            fulls[part].at[origin], fulls[part].at[origin],
            line_send.at[side, hop, part], line_recv.at[side, hop, part], {"dp": me ^ 1},
        )

    def across(way, hop, part):
        side = 0 if way > 0 else 1
        origin = me - 2 * way * hop
        src = shards[part] if hop == 0 else fulls[part].at[origin]
        return remote(
            src, fulls[part].at[origin],
            pair_send.at[side, hop, part], pair_recv.at[side, hop, part], {"dp": me ^ 1},
        )

    def across_arriving(way, hop, part):
        side = 0 if way > 0 else 1
        origin = (me ^ 1) - 2 * way * hop
        return remote(
            fulls[part].at[origin], fulls[part].at[origin],
            pair_send.at[side, hop, part], pair_recv.at[side, hop, part], {"dp": me ^ 1},
        )

    def has(way, hop):
        behind = chip >= hop if way > 0 else chip < chips - hop
        ahead = chip < chips - 1 if way > 0 else chip >= 1
        return behind, ahead

    for part in (0, 1):
        for way in (1, -1):
            @pl.when(has(way, 0)[1])
            def _(way=way, part=part):
                along(way, 0, part).start()
    for part in (0, 1):
        across(1, 0, part).start()

    tok_copies = []

    def pick(d):
        column = jnp.transpose(jnp.broadcast_to(all_ids[d], (128, slots)))
        lane = lax.broadcasted_iota(jnp.int32, (slots, 128), 1)
        cols = [
            jnp.where(column == lane + c * 128, 1.0, 0.0).astype(bf16) for c in range(pool_rows // 128)
        ]
        chosen = jnp.concatenate(cols, axis=1)
        stage_x[d] = jnp.dot(chosen, tokens[...], preferred_element_type=f32).astype(bf16)
        stage_c[d] = jnp.dot(chosen, cot[...], preferred_element_type=f32).astype(bf16)

    own = pl.ds(pl.multiple_of(me_e * width, width), width)
    for d in range(1, n_e):
        id_copies[d].wait_recv()
        pick(d)
        for part, (stage, land) in enumerate(((stage_x, routed), (stage_c, cot_rows))):
            copy = remote(
                stage.at[d], land.at[:, own], tok_send.at[d, part], tok_recv.at[d, part], {"expert": me_e ^ d}
            )
            copy.start()
            tok_copies.append((d, part))
            pending.append(copy)
    pick(0)
    routed[:, own] = stage_x[0]
    cot_rows[:, own] = stage_c[0]
    gu_full[me] = shard_gu[...]
    dn_full[me] = shard_dn[...]

    for hop in range(chips - 1):
        for part in (0, 1):
            for way in (1, -1):
                behind, ahead = has(way, hop + 1)

                @pl.when(behind)
                def _(way=way, hop=hop, part=part):
                    arriving(way, hop, part).wait_recv()
                    across(way, hop + 1, part).start()

                @pl.when(jnp.logical_and(behind, ahead))
                def _(way=way, hop=hop, part=part):
                    along(way, hop + 1, part).start()

    for d, part in tok_copies:
        land = (routed, cot_rows)[part]
        theirs = pl.ds(pl.multiple_of((me_e ^ d) * width, width), width)
        stage = (stage_x, stage_c)[part]
        remote(
            stage.at[d], land.at[:, theirs], tok_send.at[d, part], tok_recv.at[d, part], {"expert": me_e ^ d}
        ).wait_recv()
    for part in (0, 1):
        across_arriving(1, 0, part).wait_recv()
        across(1, 0, part).wait_send()
    for hop in range(chips):
        for part in (0, 1):
            for way in (1, -1):
                behind, ahead = has(way, hop)

                @pl.when(jnp.logical_and(behind, ahead))
                def _(way=way, hop=hop, part=part):
                    along(way, hop, part).wait_send()

                if hop:
                    @pl.when(behind)
                    def _(way=way, hop=hop, part=part):
                        across_arriving(way, hop, part).wait_recv()
                        across(way, hop, part).wait_send()
    for copy in pending:
        copy.wait_send()


def gathered(ids, tokens, cot, shard_gu, shard_dn, n_e, n_dp):
    bf16 = jnp.bfloat16
    slots, width = ids.shape[1], tokens.shape[1]
    chips = n_dp // 2
    vmem = pl.BlockSpec(memory_space=pltpu.VMEM)
    dma = pltpu.SemaphoreType.DMA
    return pl.pallas_call(
        functools.partial(gather_kernel, n_e, n_dp),
        out_shape=(
            jax.ShapeDtypeStruct((slots, n_e * width), bf16),
            jax.ShapeDtypeStruct((slots, n_e * width), bf16),
            jax.ShapeDtypeStruct((n_dp, *shard_gu.shape), bf16),
            jax.ShapeDtypeStruct((n_dp, *shard_dn.shape), bf16),
            jax.ShapeDtypeStruct((n_e, *ids.shape), jnp.int32),
        ),
        in_specs=[vmem] * 5,
        out_specs=(vmem,) * 5,
        scratch_shapes=[
            pltpu.VMEM((n_e, slots, width), bf16),
            pltpu.VMEM((n_e, slots, width), bf16),
            dma((n_e,)), dma((n_e,)), dma((n_e, 2)), dma((n_e, 2)),
            dma((2, chips, 2)), dma((2, chips, 2)), dma((2, chips, 2)), dma((2, chips, 2)),
        ],
        compiler_params=pltpu.CompilerParams(
            collective_id=2, has_side_effects=True, vmem_limit_bytes=60 * 1024 * 1024
        ),
    )(ids, tokens, cot, shard_gu, shard_dn)


def local(
    pool_tokens,
    pool_cotangent,
    token_ids,
    route_weights,
    gate_weight,
    up_weight,
    down_weight,
    momentum_gate,
    momentum_up,
    momentum_down,
):
    bf16, f32 = jnp.bfloat16, jnp.float32
    n_e = lax.axis_size("expert")
    n_dp = lax.axis_size("dp")
    pool_rows = pool_tokens.shape[0]
    slots = token_ids.shape[1]
    hid = gate_weight.shape[2]
    shard_gu = jnp.concatenate([gate_weight[0], up_weight[0]], axis=1).astype(bf16)
    routed, cot_rows, gu_full, down_full, ids_back = gathered(
        token_ids, pool_tokens, pool_cotangent, shard_gu, down_weight[0].astype(bf16), n_e, n_dp
    )
    gu_full = gu_full.reshape(-1, 2 * hid)
    down_full = down_full.reshape(hid, -1)

    route = route_weights[0]
    scaled_cot = (route[:, None] * cot_rows.astype(f32)).astype(bf16)
    pre = dot(routed, gu_full, ((1,), (0,)))
    gate_pre, up_pre = pre[:, :hid], pre[:, hid:]
    sig = jax.nn.sigmoid(gate_pre)
    act = gate_pre * sig
    hidden = (act * up_pre).astype(bf16)
    hidden_grad = dot(scaled_cot, down_full, ((1,), (1,)))
    gate_grad = (hidden_grad * up_pre * sig * (1.0 + gate_pre * (1.0 - sig))).astype(bf16)
    up_grad = (hidden_grad * act).astype(bf16)
    both_grad = jnp.concatenate([gate_grad, up_grad], axis=1)

    me = lax.axis_index("dp")
    own_bit = me & 1
    rows_gu = gate_weight.shape[1]
    rows_d = down_weight.shape[1]
    routed_v = routed.reshape(slots, n_dp // 2, 2, rows_gu)
    hidden_v = hidden.reshape(slots, n_dp // 2, 2, rows_d)

    def half(bit, kind):
        left = lax.dynamic_index_in_dim(routed_v, bit, 2, keepdims=False).reshape(slots, -1)
        left_d = lax.dynamic_index_in_dim(hidden_v, bit, 2, keepdims=False).reshape(slots, -1)
        gu = (dot(left, both_grad, ((0,), (0,))) / slots).astype(kind)
        dn = (dot(left_d, scaled_cot, ((0,), (0,))) / slots).astype(kind)
        return gu.reshape(n_dp // 2, rows_gu, -1), dn.reshape(n_dp // 2, rows_d, -1)

    sent = half(1 - own_bit, bf16)
    kept = half(own_bit, f32)
    slot_grad = dot(both_grad, gu_full, ((1,), (1,)), bf16)
    pool_grad, fin_gu, fin_dn = merged(sent, kept, slot_grad, ids_back.reshape(1, -1), pool_rows, n_e, n_dp, hid)

    next_gate = momentum_decay * momentum_gate[0] + fin_gu[:, :hid]
    next_up = momentum_decay * momentum_up[0] + fin_gu[:, hid:]
    next_down = momentum_decay * momentum_down[0] + fin_dn
    new_gate = gate_weight[0] - learning_rate * next_gate
    new_up = up_weight[0] - learning_rate * next_up
    new_down = down_weight[0] - learning_rate * next_down
    return (
        new_gate[None],
        new_up[None],
        new_down[None],
        next_gate[None],
        next_up[None],
        next_down[None],
        pool_grad,
    )


def solution(mesh):
    in_specs = (
        P("dp", "expert"),
        P("dp", "expert"),
        P("expert", "dp"),
        P("expert", "dp"),
        P("expert", "dp", None),
        P("expert", "dp", None),
        P("expert", "dp", None),
        P("expert", "dp", None),
        P("expert", "dp", None),
        P("expert", "dp", None),
    )
    out_specs = (
        P("expert", "dp", None),
        P("expert", "dp", None),
        P("expert", "dp", None),
        P("expert", "dp", None),
        P("expert", "dp", None),
        P("expert", "dp", None),
        P("dp", "expert"),
    )
    return jax.shard_map(local, mesh=mesh, in_specs=in_specs, out_specs=out_specs, check_vma=False)
```
